32 devices in a mesh: dp: 8 (over y, x, core), tensor: 4 (over z).
Axes of the slice: x: 2, y: 2, z: 4, core: 2. Of those that a mesh axis runs over, the one named last changes fastest.
Arguments:
- hidden: bfloat16 [1024, 8192], P('dp')
- q_weight: float32 [8192, 4096], P(('dp', 'tensor')), may hold values from -0.0625 to 0.0625
- k_weight: float32 [8192, 1024], P(('dp', 'tensor')), may hold values from -0.0625 to 0.0625
- v_weight: float32 [8192, 1024], P(('dp', 'tensor')), may hold values from -0.0625 to 0.0625
- o_weight: float32 [8192, 4096], P(('dp', 'tensor')), may hold values from -0.09375 to 0.09375
- input_gain: float32 [8192], replicated, may hold values from 0.25 to 1.75
- post_gain: float32 [8192], replicated, may hold values from 0.25 to 1.75
- key_cache: bfloat16 [1024, 64, 8, 128], P('dp', None, 'tensor'), may hold values from -1000 to 1000
- value_cache: bfloat16 [1024, 64, 8, 128], P('dp', None, 'tensor'), may hold values from -6 to 6
- lengths: int32 [1024], P('dp'), may hold values from 1 to 64
Outputs:
- new_hidden: bfloat16 [1024, 8192], P('dp')
- normed: bfloat16 [1024, 8192], P('dp')
- fresh_token_keys: bfloat16 [1024, 8, 128], P('dp', 'tensor')
- new_values: bfloat16 [1024, 8, 128], P('dp', 'tensor')
The draws below stay inside these ranges and needn't reach their ends.
All inputs are finite; a program needn't handle non-finite values.
Results may differ from the reference program's by a relative error of at most 0.012.
The reference program's roundings to bfloat16 on the way count: a program that leaves them out, or rounds other values in their place, can miss the bound.
Values may be sent and summed in bfloat16 or wider, within the bound.
A program may use at most 128 MiB of HBM per device.

```python
import math
import jax
import jax.numpy as jnp
from jax import lax

D = 8192
HEADS = 32
KV_HEADS = 8
HEAD_DIM = 128
CACHE = 64
QD = 4096
KD = 1024
GROUP = 4
BATCH = 1024


def draw_hidden(key, part):
    key_base, key_rows, key_column_slice = jax.random.split(key, 3)
    base = jax.random.normal(key_base, (BATCH, D), jnp.float32)
    row_scale = jnp.exp(jax.random.uniform(key_rows, (BATCH, 1), jnp.float32) * math.log(10.0))
    rising = jnp.exp(jnp.arange(D, dtype=jnp.float32)[None, :] / D * math.log(3.0))
    column_scale = jnp.exp(jax.random.uniform(key_column_slice, (1, D), jnp.float32) * math.log(10.0)) * rising
    return (0.03 * base * row_scale * column_scale).astype(jnp.bfloat16)


def draw_key_cache(key, part):
    key_base = jax.random.fold_in(key, 0)
    shape_full = (BATCH, CACHE, KV_HEADS, HEAD_DIM)
    base = jax.random.normal(key_base, shape_full, jnp.float32)
    return base.astype(jnp.bfloat16)


def touch_ends(entries, rng, low, top_value):
    longest = entries.shape.index(max(entries.shape))
    spots = []
    for shift in (0, 1):
        where = [jax.random.randint(jax.random.fold_in(rng, axis), (), 0, length) for axis, length in enumerate(entries.shape)]
        where[longest] = (where[longest] + shift) % entries.shape[longest]
        spots.append(tuple(where))
    return entries.at[spots[0]].set(low).at[spots[1]].set(top_value)


def block_scale(stream_key, shape, shards, least, top_value):
    loudness = 1.0
    for dim, shards_of in shards:
        heights = jax.random.uniform(jax.random.fold_in(jax.random.fold_in(stream_key, 6), dim), (shards_of,), jnp.float32, least / len(shards), top_value / len(shards))
        loudness = loudness * jnp.repeat(jnp.exp(heights), shape[dim] // shards_of).reshape((-1,) + (1,) * (len(shape) - 1 - dim))
    return loudness


def scatter_about(rng, dims, scale, reach, cuts=(), kind=jnp.bfloat16):
    values = jax.random.normal(rng, dims, jnp.float32) * scale
    if len(cuts) > 0:
        values = block_scale(rng, dims, cuts, -0.22, 0.18) * values
    return jnp.clip(values, min=-reach, max=reach).astype(kind)


def setup_inputs(seed: int = 0) -> dict:
    arg_keys = jax.random.split(jax.random.key(seed), 11)
    return {
        "hidden": draw_hidden(jax.random.fold_in(arg_keys[10], 71), 0),
        "q_weight": scatter_about(arg_keys[1], (D, QD), D ** -0.5, 0.0625, ((0, 32),), jnp.float32),
        "k_weight": scatter_about(arg_keys[2], (D, KD), D ** -0.5, 0.0625, ((0, 32),), jnp.float32),
        "v_weight": scatter_about(arg_keys[3], (D, KD), D ** -0.5, 0.0625, ((0, 32),), jnp.float32),
        "o_weight": scatter_about(arg_keys[4], (D, QD), QD ** -0.5, 0.09375, ((0, 32),), jnp.float32),
        "input_gain": jnp.clip(1.0 + 0.15 * jax.random.normal(arg_keys[5], (D,), jnp.float32), 0.25, 1.75),
        "post_gain": jnp.clip(1.0 + 0.15 * jax.random.normal(arg_keys[6], (D,), jnp.float32), 0.25, 1.75),
        "key_cache": draw_key_cache(jax.random.fold_in(arg_keys[10], 71), 0),
        "value_cache": scatter_about(arg_keys[8], (BATCH, CACHE, KV_HEADS, HEAD_DIM), 1.0, 6.0, ((0, 8), (2, 4))),
        "lengths": touch_ends(jax.random.randint(arg_keys[9], (BATCH,), 1, CACHE + 1), jax.random.fold_in(arg_keys[9], 1), 1, CACHE).astype(jnp.int32),
    }


epsilon = 1e-05
rope_base = 500000.0

def rms_gain(values, gain_vector):
    mean_square = lax.optimization_barrier(jnp.mean(values * values, axis=-1, keepdims=True))
    return values * lax.rsqrt(mean_square + epsilon) * gain_vector

def rotate(values, positions):
    half_dim = values.shape[-1] // 2
    index_row = jnp.arange(half_dim, dtype=jnp.float32)
    frequency = jnp.exp(-math.log(rope_base) * index_row / half_dim)
    angle = positions.astype(jnp.float32)[:, None, None] * frequency[None, None, :]
    first_half = values[..., :half_dim]
    second_half = values[..., half_dim:]
    return jnp.concatenate([first_half * jnp.cos(angle) - second_half * jnp.sin(angle), second_half * jnp.cos(angle) + first_half * jnp.sin(angle)], axis=-1)

def reference(hidden, q_weight, k_weight, v_weight, o_weight, input_gain, post_gain, key_cache, value_cache, lengths):
    w_query = q_weight.astype(jnp.bfloat16)
    w_key = k_weight.astype(jnp.bfloat16)
    value_matrix = v_weight.astype(jnp.bfloat16)
    w_out = o_weight.astype(jnp.bfloat16)
    row_count = hidden.shape[0]
    normal_in = rms_gain(hidden.astype(jnp.float32), input_gain).astype(jnp.bfloat16)
    query = jnp.dot(normal_in, w_query, preferred_element_type=jnp.float32)
    key_part = jnp.dot(normal_in, w_key, preferred_element_type=jnp.float32)
    value_part = jnp.dot(normal_in, value_matrix, preferred_element_type=jnp.float32)
    query_b = rotate(query.reshape(row_count, HEADS, HEAD_DIM), lengths).astype(jnp.bfloat16)
    fresh_token_keys = rotate(key_part.reshape(row_count, KV_HEADS, HEAD_DIM), lengths).astype(jnp.bfloat16)
    new_values = value_part.reshape(row_count, KV_HEADS, HEAD_DIM).astype(jnp.bfloat16)
    grouped_heads = query_b.astype(jnp.float32).reshape(row_count, KV_HEADS, GROUP, HEAD_DIM)
    reciprocal_root = 1.0 / math.sqrt(HEAD_DIM)
    scores = jnp.einsum('bkgd,blkd->bkgl', grouped_heads, key_cache.astype(jnp.float32)) * reciprocal_root
    self_token_score = jnp.einsum('lfxa,lfa->lfx', grouped_heads, fresh_token_keys.astype(jnp.float32)) * reciprocal_root
    visible = jnp.arange(CACHE, dtype=jnp.int32)[None, :] < lengths.astype(jnp.int32)[:, None]
    scores = jnp.where(visible[:, None, None, :], scores, -jnp.inf)
    largest = jnp.maximum(lax.optimization_barrier(jnp.max(scores, axis=-1)), self_token_score)
    kept_exp = jnp.exp(scores - largest[..., None])
    own_exp = jnp.exp(self_token_score - largest)
    softmax_divisor = lax.optimization_barrier(jnp.sum(kept_exp, axis=-1)) + own_exp
    weights_kept = (kept_exp / softmax_divisor[..., None]).astype(jnp.bfloat16)
    own_weight = (own_exp / softmax_divisor).astype(jnp.bfloat16)
    attended = jnp.einsum('bkgl,blkd->bkgd', weights_kept.astype(jnp.float32), value_cache.astype(jnp.float32))
    attended = attended + own_weight.astype(jnp.float32)[..., None] * new_values.astype(jnp.float32)[:, :, None, :]
    attended = attended.reshape(row_count, HEADS * HEAD_DIM).astype(jnp.bfloat16)
    mixed = jnp.dot(attended, w_out.T, preferred_element_type=jnp.float32)
    residual = hidden.astype(jnp.float32) + mixed
    new_hidden = residual.astype(jnp.bfloat16)
    normed = rms_gain(residual, post_gain).astype(jnp.bfloat16)
    return (new_hidden, normed, fresh_token_keys, new_values)
```

```python
import functools
import math

import jax
import jax.numpy as jnp
from jax import lax
from jax.experimental import pallas as pl
from jax.experimental.pallas import tpu as pltpu
from jax.sharding import PartitionSpec as P

HEADS = 32
KV_HEADS = 8
HEAD_DIM = 128

CHUNKS = 1

BF = jnp.bfloat16
F32 = jnp.float32

epsilon = 1e-05
rope_base = 500000.0


def rms_gain(values, gain_vector):
    mean_square = jnp.mean(values * values, axis=-1, keepdims=True)
    return values * lax.rsqrt(mean_square + epsilon) * gain_vector


def rotate(values, positions):
    half_dim = values.shape[-1] // 2
    index_row = jnp.arange(half_dim, dtype=jnp.float32)
    frequency = jnp.exp(-math.log(rope_base) * index_row / half_dim)
    angle = positions.astype(jnp.float32)[:, None, None] * frequency[None, None, :]
    first_half = values[..., :half_dim]
    second_half = values[..., half_dim:]
    return jnp.concatenate(
        [
            first_half * jnp.cos(angle) - second_half * jnp.sin(angle),
            second_half * jnp.cos(angle) + first_half * jnp.sin(angle),
        ],
        axis=-1,
    )


def attend(query_b, fresh_token_keys, new_values, key_cache, value_cache, lengths):
    row_count, kv_count = (fresh_token_keys.shape[0], fresh_token_keys.shape[1])
    grouped_heads = query_b.reshape(row_count, kv_count, -1, HEAD_DIM)
    reciprocal_root = 1.0 / math.sqrt(HEAD_DIM)
    scores = (
        jnp.einsum("bkgd,blkd->bkgl", grouped_heads, key_cache, preferred_element_type=jnp.float32)
        * reciprocal_root
    )
    self_token_score = (
        jnp.einsum(
            "lfxa,lfa->lfx", grouped_heads, fresh_token_keys, preferred_element_type=jnp.float32
        )
        * reciprocal_root
    )
    visible = jnp.arange(key_cache.shape[1], dtype=jnp.int32)[None, :] < lengths[:, None]
    scores = jnp.where(visible[:, None, None, :], scores, -jnp.inf)
    largest = jnp.maximum(jnp.max(scores, axis=-1), self_token_score)
    kept_exp = jnp.exp(scores - largest[..., None])
    own_exp = jnp.exp(self_token_score - largest)
    softmax_divisor = jnp.sum(kept_exp, axis=-1) + own_exp
    weights_kept = (kept_exp / softmax_divisor[..., None]).astype(jnp.bfloat16)
    own_weight = (own_exp / softmax_divisor).astype(jnp.bfloat16)
    attended = jnp.einsum(
        "bkgl,blkd->bkgd", weights_kept, value_cache, preferred_element_type=jnp.float32
    )
    attended = (
        attended
        + own_weight.astype(jnp.float32)[..., None] * new_values.astype(jnp.float32)[:, :, None, :]
    )
    return attended.reshape(row_count, -1).astype(jnp.bfloat16)


def swap(x, axis, mask, size):
    return lax.ppermute(x, axis, [(i, i ^ mask) for i in range(size)])


def add(a, b):
    return (a.astype(F32) + b.astype(F32)).astype(BF)


def bits_of(size):
    return [1 << k for k in range(size.bit_length() - 1)]


def scatter_sum(parts, bits, axis, size):
    for b in bits:
        up = sorted(m for m in parts if m & b)
        got = swap(jnp.stack([parts[m] for m in up]), axis, b, size)
        parts = {m: add(parts[m], got[up.index(m | b)]) for m in parts if not m & b}
    return parts[0]


def gather_all(x, bits, axis, size):
    held = {0: x}
    for b in bits:
        keys = sorted(held)
        got = swap(jnp.stack([held[m] for m in keys]), axis, b, size)
        held.update({m | b: got[k] for k, m in enumerate(keys)})
    return held


def norm_pieces_kernel(nd, nt, feat, hidden_ref, gain_ref, *outs):
    me, ten = lax.axis_index("dp"), lax.axis_index("tensor")
    h = hidden_ref[...].astype(F32)
    scale = lax.rsqrt(jnp.mean(h * h, axis=-1, keepdims=True) + epsilon)
    for m in range(nd):
        at = pl.ds(pl.multiple_of(((me ^ m) * nt + ten) * feat, feat), feat)
        outs[m][...] = (hidden_ref[:, at].astype(F32) * scale * gain_ref[:, at]).astype(BF)


def norm_pieces(hidden, gain, nd, nt, feat):
    rows, width = hidden.shape
    if feat % 128:
        me, ten = lax.axis_index("dp"), lax.axis_index("tensor")
        normal_in = rms_gain(hidden.astype(F32), gain).astype(BF)
        return [
            lax.dynamic_slice_in_dim(normal_in, ((me ^ m) * nt + ten) * feat, feat, 1)
            for m in range(nd)
        ]
    tile = min(32, rows)
    return pl.pallas_call(
        functools.partial(norm_pieces_kernel, nd, nt, feat),
        grid=(rows // tile,),
        in_specs=[
            pl.BlockSpec((tile, width), lambda i: (i, 0)),
            pl.BlockSpec((1, width), lambda i: (0, 0)),
        ],
        out_specs=[pl.BlockSpec((tile, feat), lambda i: (i, 0))] * nd,
        out_shape=[jax.ShapeDtypeStruct((rows, feat), BF)] * nd,
        cost_estimate=pl.CostEstimate(flops=rows * width * 20, bytes_accessed=4 * rows * width, transcendentals=0),
    )(hidden, gain.reshape(1, width))


def finish_kernel(nd, nt, feat, masks, hidden_ref, gain_ref, *refs):
    blocks, (new_ref, normed_ref), (res, squares) = refs[: len(masks)], refs[-4:-2], refs[-2:]
    me, ten = lax.axis_index("dp"), lax.axis_index("tensor")
    squares[...] = jnp.zeros_like(squares)
    for ref, group in zip(blocks, masks):
        for k, s in enumerate(group):
            for m in range(nd):
                col = ((me ^ m) * nt + (ten ^ s)) * feat
                at = pl.ds(pl.multiple_of(col, feat), feat)
                r = hidden_ref[:, at].astype(F32) + ref[k, m].astype(F32)
                new_ref[:, at] = r.astype(BF)
                res[:, at] = r
                squares[...] += r * r
    mean = jnp.sum(squares[...], axis=-1, keepdims=True) / res.shape[1]
    normed_ref[...] = (res[...] * lax.rsqrt(mean + epsilon) * gain_ref[...]).astype(BF)


def finish(hidden, gain, first, count, stages, nd, nt, feat, before):
    rows, width = hidden.shape
    tile = min(32, count)
    base = first // tile
    masks = [g for g, _ in stages]
    row = pl.BlockSpec((tile, width), lambda i: (i + base, 0))
    specs = [row, pl.BlockSpec((1, width), lambda i: (0, 0))]
    for g, _ in stages:
        specs.append(pl.BlockSpec((len(g), nd, tile, feat), lambda i: (0, 0, i, 0)))
    args = [hidden, gain.reshape(1, width)] + [x for _, x in stages]
    alias = {}
    if before is not None:
        alias = {len(args): 0, len(args) + 1: 1}
        specs += [pl.BlockSpec(memory_space=pl.ANY)] * 2
        args += list(before)
    return pl.pallas_call(
        functools.partial(finish_kernel, nd, nt, feat, masks),
        grid=(count // tile,),
        in_specs=specs,
        out_specs=[row, row],
        out_shape=[jax.ShapeDtypeStruct((rows, width), BF)] * 2,
        scratch_shapes=[pltpu.VMEM((tile, width), F32), pltpu.VMEM((tile, feat), F32)],
        input_output_aliases=alias,
        cost_estimate=pl.CostEstimate(flops=count * width * 20, bytes_accessed=8 * count * width, transcendentals=0),
    )(*args)


def shards(
    hidden,
    q_weight,
    k_weight,
    v_weight,
    o_weight,
    input_gain,
    post_gain,
    key_cache,
    value_cache,
    lengths,
):
    nt = lax.axis_size("tensor")
    nd = lax.axis_size("dp")
    me, ten = lax.axis_index("dp"), lax.axis_index("tensor")
    rows, width = hidden.shape
    heads_here, kv_here = HEADS // nt, KV_HEADS // nt
    qc, kc = heads_here * HEAD_DIM, kv_here * HEAD_DIM
    feat = q_weight.shape[0]
    low, high = [1], bits_of(nd)[1:]
    orders = (low + high, low + high[::-1])
    odd = [m for m in range(nd) if m & 1]
    even = [m for m in range(nd) if not m & 1]
    count = rows // CHUNKS

    def columns(w, s, n):
        return lax.dynamic_slice_in_dim(w, (ten ^ s) * n, n, 1).astype(BF)

    pieces = norm_pieces(hidden, input_gain, nd, nt, feat)
    pieces = [swap(p, "dp", m, nd) if m else p for m, p in enumerate(pieces)]
    w_in = [
        jnp.concatenate(
            [columns(q_weight, s, qc), columns(k_weight, s, kc), columns(v_weight, s, kc)], axis=1
        )
        for s in range(nt)
    ]
    w_out = [columns(o_weight, s, qc) for s in range(nt)]

    fresh, values, outs = [], [], None
    for c in range(CHUNKS):
        r0 = c * count
        cut = [p[r0 : r0 + count] for p in pieces]
        lhs_odd = jnp.concatenate([cut[m] for m in odd])
        lhs_even = jnp.concatenate([cut[m] for m in even])
        total = None
        for k, s in enumerate(reversed(range(nt))):
            away = jnp.dot(lhs_odd, w_in[s], preferred_element_type=F32).astype(BF)
            got = swap(away, "dp", 1, nd)
            acc = jnp.dot(lhs_even, w_in[s], preferred_element_type=F32) + got.astype(F32)
            acc = acc.astype(BF).reshape(len(even), count, -1)
            parts = {m: acc[j] for j, m in enumerate(even)}
            part = scatter_sum(parts, orders[k % 2][1:], "dp", nd)
            part = (swap(part, "tensor", s, nt) if s else part).astype(F32)
            total = part if total is None else total + part
        query, key_part, value_part = total[:, :qc], total[:, qc : qc + kc], total[:, qc + kc :]

        here = slice(r0, r0 + count)
        query_b = rotate(query.reshape(count, heads_here, HEAD_DIM), lengths[here]).astype(BF)
        keys = rotate(key_part.reshape(count, kv_here, HEAD_DIM), lengths[here]).astype(BF)
        news = value_part.reshape(count, kv_here, HEAD_DIM).astype(BF)
        fresh.append(keys)
        values.append(news)
        attended = attend(
            query_b, keys, news, key_cache[here], value_cache[here], lengths[here]
        )

        by_tensor = gather_all(attended, bits_of(nt)[::-1], "tensor", nt)
        product = None
        for k, s in enumerate(sorted(by_tensor, key=lambda s: (s & 1, s))):
            blocks = gather_all(by_tensor[s], orders[k % 2][1:] + low, "dp", nd)
            lhs = jnp.concatenate([blocks[m] for m in range(nd)])
            term = lax.dot_general(
                lhs, w_out[s], (((1,), (1,)), ((), ())), preferred_element_type=F32
            )
            product = term if product is None else product + term
        product = product.astype(BF).reshape(nd, count, feat)
        mine = jnp.stack([swap(product[m], "dp", m, nd) if m else product[0] for m in range(nd)])
        if feat % 128:
            for b in bits_of(nd):
                v = mine.reshape(nd // (2 * b), 2, b, count, feat)
                mine = jnp.where((me & b) != 0, v[:, ::-1], v).reshape(nd, count, feat)
            mine = mine[None]
            for b in bits_of(nt)[::-1]:
                got = swap(mine, "tensor", b, nt)
                first = jnp.where((ten & b) != 0, got, mine)
                second = jnp.where((ten & b) != 0, mine, got)
                mine = jnp.stack([first, second], axis=1).reshape((-1,) + mine.shape[1:])
            mixed = mine.transpose(2, 1, 0, 3).reshape(count, width).astype(F32)
            residual = hidden[here].astype(F32) + mixed
            pair = (residual.astype(BF), rms_gain(residual, post_gain).astype(BF))
            outs = pair if outs is None else tuple(jnp.concatenate(z) for z in zip(outs, pair))
        else:
            stages = [((0,), mine[None])]
            for b in bits_of(nt)[::-1]:
                stages += [(tuple(s | b for s in g), swap(x, "tensor", b, nt)) for g, x in stages]
            outs = finish(hidden, post_gain, r0, count, stages, nd, nt, feat, outs)
    return (outs[0], outs[1], jnp.concatenate(fresh), jnp.concatenate(values))


def solution(mesh):
    in_specs = (
        P("dp", None),
        P(("dp", "tensor"), None),
        P(("dp", "tensor"), None),
        P(("dp", "tensor"), None),
        P(("dp", "tensor"), None),
        P(),
        P(),
        P("dp", None, "tensor", None),
        P("dp", None, "tensor", None),
        P("dp"),
    )
    out_specs = (P("dp", None), P("dp", None), P("dp", "tensor", None), P("dp", "tensor", None))
    return jax.shard_map(shards, mesh=mesh, in_specs=in_specs, out_specs=out_specs, check_vma=False)
```

```python
import functools
import math

import jax
import jax.numpy as jnp
from jax import lax
from jax.experimental import pallas as pl
from jax.experimental.pallas import tpu as pltpu
from jax.sharding import PartitionSpec as P

HEADS = 32
KV_HEADS = 8
HEAD_DIM = 128

CHUNKS = 1

BF = jnp.bfloat16
F32 = jnp.float32

epsilon = 1e-05
rope_base = 500000.0


def rms_gain(values, gain_vector):
    mean_square = jnp.mean(values * values, axis=-1, keepdims=True)
    return values * lax.rsqrt(mean_square + epsilon) * gain_vector


def rotate(values, positions):
    half_dim = values.shape[-1] // 2
    index_row = jnp.arange(half_dim, dtype=jnp.float32)
    frequency = jnp.exp(-math.log(rope_base) * index_row / half_dim)
    angle = positions.astype(jnp.float32)[:, None, None] * frequency[None, None, :]
    first_half = values[..., :half_dim]
    second_half = values[..., half_dim:]
    return jnp.concatenate(
        [
            first_half * jnp.cos(angle) - second_half * jnp.sin(angle),
            second_half * jnp.cos(angle) + first_half * jnp.sin(angle),
        ],
        axis=-1,
    )


def attend(query_b, fresh_token_keys, new_values, key_cache, value_cache, lengths):
    row_count, kv_count = (fresh_token_keys.shape[0], fresh_token_keys.shape[1])
    grouped_heads = query_b.reshape(row_count, kv_count, -1, HEAD_DIM)
    reciprocal_root = 1.0 / math.sqrt(HEAD_DIM)
    scores = (
        jnp.einsum("bkgd,blkd->bkgl", grouped_heads, key_cache, preferred_element_type=jnp.float32)
        * reciprocal_root
    )
    self_token_score = (
        jnp.einsum(
            "lfxa,lfa->lfx", grouped_heads, fresh_token_keys, preferred_element_type=jnp.float32
        )
        * reciprocal_root
    )
    visible = jnp.arange(key_cache.shape[1], dtype=jnp.int32)[None, :] < lengths[:, None]
    scores = jnp.where(visible[:, None, None, :], scores, -jnp.inf)
    largest = jnp.maximum(jnp.max(scores, axis=-1), self_token_score)
    kept_exp = jnp.exp(scores - largest[..., None])
    own_exp = jnp.exp(self_token_score - largest)
    softmax_divisor = jnp.sum(kept_exp, axis=-1) + own_exp
    weights_kept = (kept_exp / softmax_divisor[..., None]).astype(jnp.bfloat16)
    own_weight = (own_exp / softmax_divisor).astype(jnp.bfloat16)
    attended = jnp.einsum(
        "bkgl,blkd->bkgd", weights_kept, value_cache, preferred_element_type=jnp.float32
    )
    attended = (
        attended
        + own_weight.astype(jnp.float32)[..., None] * new_values.astype(jnp.float32)[:, :, None, :]
    )
    return attended.reshape(row_count, -1).astype(jnp.bfloat16)


def swap(x, axis, mask, size):
    return lax.ppermute(x, axis, [(i, i ^ mask) for i in range(size)])


def add(a, b):
    return (a.astype(F32) + b.astype(F32)).astype(BF)


def bits_of(size):
    return [1 << k for k in range(size.bit_length() - 1)]


def scatter_sum(parts, bits, axis, size):
    for b in bits:
        up = sorted(m for m in parts if m & b)
        got = swap(jnp.stack([parts[m] for m in up]), axis, b, size)
        parts = {m: add(parts[m], got[up.index(m | b)]) for m in parts if not m & b}
    return parts[0]


def gather_all(x, bits, axis, size):
    held = {0: x}
    for b in bits:
        keys = sorted(held)
        got = swap(jnp.stack([held[m] for m in keys]), axis, b, size)
        held.update({m | b: got[k] for k, m in enumerate(keys)})
    return held


def norm_pieces_kernel(nd, nt, feat, hidden_ref, gain_ref, *outs):
    me, ten = lax.axis_index("dp"), lax.axis_index("tensor")
    h = hidden_ref[...].astype(F32)
    scale = lax.rsqrt(jnp.mean(h * h, axis=-1, keepdims=True) + epsilon)
    for m in range(nd):
        at = pl.ds(pl.multiple_of(((me ^ m) * nt + ten) * feat, feat), feat)
        outs[m][...] = (hidden_ref[:, at].astype(F32) * scale * gain_ref[:, at]).astype(BF)


def norm_pieces(hidden, gain, nd, nt, feat):
    rows, width = hidden.shape
    if feat % 128:
        me, ten = lax.axis_index("dp"), lax.axis_index("tensor")
        normal_in = rms_gain(hidden.astype(F32), gain).astype(BF)
        return [
            lax.dynamic_slice_in_dim(normal_in, ((me ^ m) * nt + ten) * feat, feat, 1)
            for m in range(nd)
        ]
    tile = min(32, rows)
    return pl.pallas_call(
        functools.partial(norm_pieces_kernel, nd, nt, feat),
        grid=(rows // tile,),
        in_specs=[
            pl.BlockSpec((tile, width), lambda i: (i, 0)),
            pl.BlockSpec((1, width), lambda i: (0, 0)),
        ],
        out_specs=[pl.BlockSpec((tile, feat), lambda i: (i, 0))] * nd,
        out_shape=[jax.ShapeDtypeStruct((rows, feat), BF)] * nd,
        cost_estimate=pl.CostEstimate(flops=rows * width * 20, bytes_accessed=4 * rows * width, transcendentals=0),
    )(hidden, gain.reshape(1, width))


def finish_kernel(nd, nt, feat, masks, hidden_ref, gain_ref, *refs):
    blocks, (new_ref, normed_ref), (res, squares) = refs[: len(masks)], refs[-4:-2], refs[-2:]
    me, ten = lax.axis_index("dp"), lax.axis_index("tensor")
    squares[...] = jnp.zeros_like(squares)
    for ref, group in zip(blocks, masks):
        for k, s in enumerate(group):
            for m in range(nd):
                col = ((me ^ m) * nt + (ten ^ s)) * feat
                at = pl.ds(pl.multiple_of(col, feat), feat)
                r = hidden_ref[:, at].astype(F32) + ref[k, m].astype(F32)
                new_ref[:, at] = r.astype(BF)
                res[:, at] = r
                squares[...] += r * r
    mean = jnp.sum(squares[...], axis=-1, keepdims=True) / res.shape[1]
    normed_ref[...] = (res[...] * lax.rsqrt(mean + epsilon) * gain_ref[...]).astype(BF)


def finish(hidden, gain, first, count, stages, nd, nt, feat, before):
    rows, width = hidden.shape
    tile = min(32, count)
    base = first // tile
    masks = [g for g, _ in stages]
    row = pl.BlockSpec((tile, width), lambda i: (i + base, 0))
    specs = [row, pl.BlockSpec((1, width), lambda i: (0, 0))]
    for g, _ in stages:
        specs.append(pl.BlockSpec((len(g), nd, tile, feat), lambda i: (0, 0, i, 0)))
    args = [hidden, gain.reshape(1, width)] + [x for _, x in stages]
    alias = {}
    if before is not None:
        alias = {len(args): 0, len(args) + 1: 1}
        specs += [pl.BlockSpec(memory_space=pl.ANY)] * 2
        args += list(before)
    return pl.pallas_call(
        functools.partial(finish_kernel, nd, nt, feat, masks),
        grid=(count // tile,),
        in_specs=specs,
        out_specs=[row, row],
        out_shape=[jax.ShapeDtypeStruct((rows, width), BF)] * 2,
        scratch_shapes=[pltpu.VMEM((tile, width), F32), pltpu.VMEM((tile, feat), F32)],
        input_output_aliases=alias,
        cost_estimate=pl.CostEstimate(flops=count * width * 20, bytes_accessed=8 * count * width, transcendentals=0),
    )(*args)


def flip(i, mask):
    for b in (1, 2, 4, 8, 16, 32, 64):
        if mask & b:
            i = i + b - 2 * b * ((i // b) % 2)
    return i


def project_kernel(nd, nt, own_ref, *refs):
    w_refs, (fin, att, prod, zs, zr, ds, dr, ps, pr, fs, fr) = refs[:nt], refs[nt:]
    me, ten = lax.axis_index("dp"), lax.axis_index("tensor")
    rows = own_ref.shape[0]
    half = rows // 2
    evens = list(range(0, nd, 2))
    slot = {m: k for k, m in enumerate(evens + [m + 1 for m in evens])}
    high, zbits = bits_of(nd)[1:], bits_of(nt)[::-1]
    orders = (high + [1], high[::-1] + [1])
    started = []

    def send(src, dst, ssem, rsem, where):
        copy = pltpu.make_async_remote_copy(
            src_ref=src, dst_ref=dst, send_sem=ssem, recv_sem=rsem,
            device_id=where, device_id_type=pl.DeviceIdType.MESH,
        )
        copy.start()
        started.append(copy)

    def await_into(dst, sem):
        pltpu.make_async_remote_copy(
            src_ref=dst, dst_ref=dst, send_sem=sem, recv_sem=sem,
            device_id={"dp": me}, device_id_type=pl.DeviceIdType.MESH,
        ).wait_recv()

    barrier = pltpu.get_barrier_semaphore()
    for m in range(1, nd):
        pl.semaphore_signal(
            barrier, inc=1, device_id={"dp": flip(me, m)}, device_id_type=pl.DeviceIdType.MESH
        )
    for b in zbits:
        pl.semaphore_signal(
            barrier, inc=1, device_id={"tensor": flip(ten, b)}, device_id_type=pl.DeviceIdType.MESH
        )
    pl.semaphore_wait(barrier, nd - 1 + len(zbits))

    def block(m, s):
        return own_ref if m == 0 and s == 0 else att.at[s, slot[m]]

    def z_sends(s):
        for b in zbits:
            if b < (s & -s) or s == 0:
                send(block(0, s), att.at[s | b, 0], zs.at[s | b], zr.at[s | b], {"tensor": flip(ten, b)})

    def dp_sends(m, s, h):
        order = orders[h]
        used = [order.index(b) for b in order if m & b]
        for b in order[max(used) + 1 if used else 0 :]:
            part = pl.ds(h * half, half)
            send(
                block(m, s).at[part], att.at[s, slot[m | b], part],
                ds.at[s, m | b, h], dr.at[s, m | b, h], {"dp": flip(me, b)},
            )

    def arrive(m, s, h):
        await_into(att.at[s, slot[m], pl.ds(h * half, half)], dr.at[s, m, h])

    def relay(s):
        for bits in (1, 2, 3, 4, 5, 6):
            for h in (0, 1):
                for m in evens:
                    used = [b for b in orders[h] if m & b]
                    if len(used) == bits:
                        arrive(m, s, h)
                        dp_sends(m, s, h)

    z_sends(0)
    for h in (0, 1):
        dp_sends(0, 0, h)
    att[0, 0] = own_ref[...]
    walk = sorted(range(nt), key=lambda s: (s & 1, s)) if nt < 4 else [0, 1, 2, 3] + list(range(4, nt))
    for k, s in enumerate(walk):
        if s:
            await_into(att.at[s, 0], zr.at[s])
            z_sends(s)
            for h in (0, 1):
                dp_sends(0, s, h)
            relay(walk[k - 1])
    relay(walk[-1])

    def multiply(first):
        group = len(evens)
        out = None
        for s in range(nt):
            lhs = att[s, first : first + group].reshape(group * rows, -1)
            term = jnp.dot(lhs, w_refs[s][...], preferred_element_type=F32)
            out = term if out is None else out + term
        return out.astype(BF).reshape(group, rows, -1)

    def hand_out(ms):
        for m in ms:
            if m:
                send(prod.at[slot[m]], fin.at[0, m], ps.at[m], pr.at[m], {"dp": flip(me, m)})

    def spread(m, s):
        for b in zbits:
            if b < (s & -s) or s == 0:
                send(fin.at[s, m], fin.at[s | b, m], fs.at[s | b, m], fr.at[s | b, m], {"tensor": flip(ten, b)})

    prod[pl.ds(0, len(evens))] = multiply(0)
    hand_out(evens)
    fin[0, 0] = prod[0]
    spread(0, 0)
    for s in walk:
        for m in evens:
            for h in (0, 1):
                arrive(m | 1, s, h)
    prod[pl.ds(len(evens), len(evens))] = multiply(len(evens))
    hand_out([m + 1 for m in evens])
    sequence = evens + [m + 1 for m in evens]
    for m in sequence:
        if m:
            await_into(fin.at[0, m], pr.at[m])
            spread(m, 0)
    for s in sorted(range(1, nt), key=lambda s: (s & 1, s)):
        for m in sequence:
            await_into(fin.at[s, m], fr.at[s, m])
            spread(m, s)
    for copy in started:
        copy.wait_send()


def project(attended, w_out, nd, nt, feat):
    rows, qc = attended.shape
    dma = pltpu.SemaphoreType.DMA
    return pl.pallas_call(
        functools.partial(project_kernel, nd, nt),
        in_specs=[pl.BlockSpec(memory_space=pltpu.VMEM)] * (1 + nt),
        out_specs=pl.BlockSpec(memory_space=pltpu.VMEM),
        out_shape=jax.ShapeDtypeStruct((nt, nd, rows, feat), BF),
        scratch_shapes=[
            pltpu.VMEM((nt, nd, rows, qc), BF),
            pltpu.VMEM((nd, rows, feat), BF),
            dma((nt,)), dma((nt,)),
            dma((nt, nd, 2)), dma((nt, nd, 2)),
            dma((nd,)), dma((nd,)),
            dma((nt, nd)), dma((nt, nd)),
        ],
        compiler_params=pltpu.CompilerParams(
            collective_id=1, has_side_effects=True, vmem_limit_bytes=48 * 1024 * 1024
        ),
    )(attended, *w_out)


def shards(
    hidden,
    q_weight,
    k_weight,
    v_weight,
    o_weight,
    input_gain,
    post_gain,
    key_cache,
    value_cache,
    lengths,
):
    nt = lax.axis_size("tensor")
    nd = lax.axis_size("dp")
    me, ten = lax.axis_index("dp"), lax.axis_index("tensor")
    rows, width = hidden.shape
    heads_here, kv_here = HEADS // nt, KV_HEADS // nt
    qc, kc = heads_here * HEAD_DIM, kv_here * HEAD_DIM
    feat = q_weight.shape[0]
    low, high = [1], bits_of(nd)[1:]
    orders = (low + high, low + high[::-1])
    odd = [m for m in range(nd) if m & 1]
    even = [m for m in range(nd) if not m & 1]
    count = rows // CHUNKS

    def columns(w, s, n):
        return lax.dynamic_slice_in_dim(w, (ten ^ s) * n, n, 1).astype(BF)

    pieces = norm_pieces(hidden, input_gain, nd, nt, feat)
    pieces = [swap(p, "dp", m, nd) if m else p for m, p in enumerate(pieces)]
    w_in = [
        jnp.concatenate(
            [columns(q_weight, s, qc), columns(k_weight, s, kc), columns(v_weight, s, kc)], axis=1
        )
        for s in range(nt)
    ]
    w_out = [columns(o_weight, s, qc) for s in range(nt)]
    if feat % 128 == 0:
        w_out = [w.T for w in w_out]

    fresh, values, outs = [], [], None
    for c in range(CHUNKS):
        r0 = c * count
        cut = [p[r0 : r0 + count] for p in pieces]
        lhs_odd = jnp.concatenate([cut[m] for m in odd])
        lhs_even = jnp.concatenate([cut[m] for m in even])
        total, behind = None, []
        for k, s in enumerate(reversed(range(nt))):
            if k and k % 2 == 0:
                held = lax.optimization_barrier((lhs_odd, lhs_even, *behind))
                lhs_odd, lhs_even, behind = held[0], held[1], []
            away = jnp.dot(lhs_odd, w_in[s], preferred_element_type=F32).astype(BF)
            got = swap(away, "dp", 1, nd)
            behind.append(got)
            acc = jnp.dot(lhs_even, w_in[s], preferred_element_type=F32) + got.astype(F32)
            acc = acc.astype(BF).reshape(len(even), count, -1)
            parts = {m: acc[j] for j, m in enumerate(even)}
            part = scatter_sum(parts, orders[k % 2][1:], "dp", nd)
            part = (swap(part, "tensor", s, nt) if s else part).astype(F32)
            total = part if total is None else total + part
        query, key_part, value_part = total[:, :qc], total[:, qc : qc + kc], total[:, qc + kc :]

        here = slice(r0, r0 + count)
        query_b = rotate(query.reshape(count, heads_here, HEAD_DIM), lengths[here]).astype(BF)
        keys = rotate(key_part.reshape(count, kv_here, HEAD_DIM), lengths[here]).astype(BF)
        news = value_part.reshape(count, kv_here, HEAD_DIM).astype(BF)
        fresh.append(keys)
        values.append(news)
        attended = attend(
            query_b, keys, news, key_cache[here], value_cache[here], lengths[here]
        )

        if feat % 128 == 0:
            mine = project(attended, w_out, nd, nt, feat)
            outs = finish(
                hidden, post_gain, r0, count, [(tuple(range(nt)), mine)], nd, nt, feat, outs
            )
            continue
        by_tensor = gather_all(attended, bits_of(nt)[::-1], "tensor", nt)
        product = None
        for k, s in enumerate(sorted(by_tensor, key=lambda s: (s & 1, s))):
            blocks = gather_all(by_tensor[s], orders[k % 2][1:] + low, "dp", nd)
            lhs = jnp.concatenate([blocks[m] for m in range(nd)])
            term = lax.dot_general(
                lhs, w_out[s], (((1,), (1,)), ((), ())), preferred_element_type=F32
            )
            product = term if product is None else product + term
        product = product.astype(BF).reshape(nd, count, feat)
        mine = jnp.stack([swap(product[m], "dp", m, nd) if m else product[0] for m in range(nd)])
        for b in bits_of(nd):
            v = mine.reshape(nd // (2 * b), 2, b, count, feat)
            mine = jnp.where((me & b) != 0, v[:, ::-1], v).reshape(nd, count, feat)
        mine = mine[None]
        for b in bits_of(nt)[::-1]:
            got = swap(mine, "tensor", b, nt)
            first = jnp.where((ten & b) != 0, got, mine)
            second = jnp.where((ten & b) != 0, mine, got)
            mine = jnp.stack([first, second], axis=1).reshape((-1,) + mine.shape[1:])
        mixed = mine.transpose(2, 1, 0, 3).reshape(count, width).astype(F32)
        residual = hidden[here].astype(F32) + mixed
        pair = (residual.astype(BF), rms_gain(residual, post_gain).astype(BF))
        outs = pair if outs is None else tuple(jnp.concatenate(z) for z in zip(outs, pair))
    return (outs[0], outs[1], jnp.concatenate(fresh), jnp.concatenate(values))


def solution(mesh):
    in_specs = (
        P("dp", None),
        P(("dp", "tensor"), None),
        P(("dp", "tensor"), None),
        P(("dp", "tensor"), None),
        P(("dp", "tensor"), None),
        P(),
        P(),
        P("dp", None, "tensor", None),
        P("dp", None, "tensor", None),
        P("dp"),
    )
    out_specs = (P("dp", None), P("dp", None), P("dp", "tensor", None), P("dp", "tensor", None))
    return jax.shard_map(shards, mesh=mesh, in_specs=in_specs, out_specs=out_specs, check_vma=False)
```
